32 devices in a mesh: zero: 2 (over core), tp: 4 (over y, x), job: 4 (over z).
Axes of the slice: x: 2, y: 2, z: 4, core: 2. Of those that a mesh axis runs over, the one named last changes fastest.
Arguments:
- w_query: float32 [16384, 4096], P(('job', 'zero'), 'tp'), parts along dimension 0, may hold values from -0.125 to 0.125
- avg_query: float32 [16384, 4096], P(('job', 'zero'), 'tp'), parts along dimension 0, may hold values from -0.09375 to 0.09375
- w_key: float32 [16384, 1024], P(('job', 'zero'), 'tp'), parts along dimension 0, may hold values from -0.125 to 0.125
- avg_key: float32 [16384, 1024], P(('job', 'zero'), 'tp'), parts along dimension 0, may hold values from -0.09375 to 0.09375
- w_value: float32 [16384, 1024], P(('job', 'zero'), 'tp'), parts along dimension 0, may hold values from -0.125 to 0.125
- avg_value: float32 [16384, 1024], P(('job', 'zero'), 'tp'), parts along dimension 0, may hold values from -0.09375 to 0.09375
- norm_train: float32 [16384], P(('job', 'zero', 'tp')), parts along dimension 0, may hold values from 0.25 to 1.75
- norm_step: float32 [16384], P(('job', 'zero', 'tp')), parts along dimension 0, may hold values from -0.3 to 0.3
Outputs:
- serve_query: bfloat16 [16384, 4096], P('job', 'tp'), parts along dimension 0
- serve_key: bfloat16 [16384, 1024], P('job', 'tp'), parts along dimension 0
- serve_value: bfloat16 [16384, 1024], P('job', 'tp'), parts along dimension 0
- column_query: float32 [16384], P(('job', 'tp')), parts along dimension 0
- column_key: float32 [4096], P(('job', 'tp')), parts along dimension 0
- column_value: float32 [4096], P(('job', 'tp')), parts along dimension 0
- serve_norm: bfloat16 [16384], P('job'), parts along dimension 0
- fresh_query: float32 [16384, 4096], P(('job', 'zero'), 'tp'), parts along dimension 0
- fresh_key: float32 [16384, 1024], P(('job', 'zero'), 'tp'), parts along dimension 0
- fresh_value: float32 [16384, 1024], P(('job', 'zero'), 'tp'), parts along dimension 0
The draws below stay inside these ranges and needn't reach their ends.
There are 4 independent parts, one for each index of `job`. The reference program is written for one: setup_inputs(seed, part) draws one part's arguments, and reference() takes and returns one part's arrays. A program takes and returns all parts, laid end to end along the dimension named above; each array names one. Nothing has to cross between parts.
All inputs are finite; a program needn't handle non-finite values.
Results may differ from the reference program's by a relative error of at most 0.001.
Values may be sent and summed in bfloat16 or wider, within the bound.
A program may use at most 128 MiB of HBM per device.

```python
import jax
import jax.numpy as jnp
from jax import lax

D_MODEL = 4096
Q_DIM = 4096
KV_DIM = 1024


def spiked(entries, rng, source, target, shards_of, factor):
    owner, partner = [(jnp.arange(entries.shape[axis_at]) // (entries.shape[axis_at] // shards_of)).reshape([-1 if axis == axis_at else 1 for axis in range(entries.ndim)]) for axis_at in (source, target)]
    chosen = jax.random.permutation(rng, shards_of)[partner]
    strong = (owner == chosen) | (owner == (partner + shards_of // 2) % shards_of)
    return jnp.where(strong, factor * entries, entries)


def levels(stream_key, extent, cuts, smallest, largest):
    factor_of, own = 1.0, jax.random.fold_in(stream_key, 6)
    for position, parts in cuts:
        heights = jnp.exp(jax.random.uniform(jax.random.fold_in(own, position), (parts,), jnp.float32, smallest / len(cuts), largest / len(cuts)))
        factor_of = factor_of * jnp.repeat(heights, extent[position] // parts).reshape([-1 if axis == position else 1 for axis in range(len(extent))])
    return factor_of


def bell_draw(key, shape, width, limit, pieces=(), kind=jnp.bfloat16):
    result = jax.random.normal(key, shape, jnp.float32) * width
    if len(pieces) > 0:
        result = levels(key, shape, pieces, -0.22, 0.18) * result
    return jnp.clip(result, min=-limit, max=limit).astype(kind)


def noise_with(key, extent, spread, bound, pieces, heavy, dtype=jnp.bfloat16):
    array = spread * jax.random.normal(key, extent, jnp.float32)
    if pieces:
        array = array * levels(key, extent, pieces, -0.22, 0.18)
    return jnp.clip(spiked(array, jax.random.fold_in(key, 3), *heavy), -bound, bound).astype(dtype)


def setup_inputs(seed: int = 0, part: int = 0) -> dict:
    splits = jax.random.split(jax.random.key(seed), 9)
    own_keys = jax.random.split(jax.random.fold_in(splits[8], part), 9)
    return {
        "w_query": noise_with(own_keys[0], (D_MODEL, Q_DIM), D_MODEL ** -0.5, 0.125, ((0, 2), (1, 4)), (0, 1, 4, 2.0), jnp.float32),
        "avg_query": bell_draw(own_keys[1], (D_MODEL, Q_DIM), D_MODEL ** -0.5, 0.09375, ((0, 2), (1, 4)), jnp.float32),
        "w_key": noise_with(own_keys[2], (D_MODEL, KV_DIM), D_MODEL ** -0.5, 0.125, ((0, 2), (1, 4)), (0, 1, 4, 2.0), jnp.float32),
        "avg_key": bell_draw(own_keys[3], (D_MODEL, KV_DIM), D_MODEL ** -0.5, 0.09375, ((0, 2), (1, 4)), jnp.float32),
        "w_value": noise_with(own_keys[4], (D_MODEL, KV_DIM), D_MODEL ** -0.5, 0.125, ((0, 2), (1, 4)), (0, 1, 4, 2.0), jnp.float32),
        "avg_value": bell_draw(own_keys[5], (D_MODEL, KV_DIM), D_MODEL ** -0.5, 0.09375, ((0, 2), (1, 4)), jnp.float32),
        "norm_train": jnp.clip(1.0 + 0.15 * jax.random.normal(own_keys[6], (D_MODEL,), jnp.float32), 0.25, 1.75),
        "norm_step": jnp.clip(jax.random.uniform(own_keys[7], (D_MODEL,), jnp.float32, -0.3, 0.3) * levels(own_keys[7], (D_MODEL,), ((0, 8),), -0.4, 0.0), -0.3, 0.3),
    }


keep_rate = 0.75

def reference(w_query, avg_query, w_key, avg_key, w_value, avg_value, norm_train, norm_step):
    fresh_query = keep_rate * avg_query + (1.0 - keep_rate) * w_query
    fresh_key = keep_rate * avg_key + (1.0 - keep_rate) * w_key
    fresh_value = keep_rate * avg_value + (1.0 - keep_rate) * w_value
    column_query = jnp.sqrt(lax.optimization_barrier(jnp.sum(fresh_query * fresh_query, axis=0)))
    serve_query = (fresh_query / column_query).astype(jnp.bfloat16)
    column_key = jnp.sqrt(lax.optimization_barrier(jnp.sum(fresh_key * fresh_key, axis=0)))
    serve_key = (fresh_key / column_key).astype(jnp.bfloat16)
    column_value = jnp.sqrt(lax.optimization_barrier(jnp.sum(fresh_value * fresh_value, axis=0)))
    serve_value = (fresh_value / column_value).astype(jnp.bfloat16)
    serve_norm = (norm_train + norm_step).astype(jnp.bfloat16)
    return (serve_query, serve_key, serve_value, column_query, column_key, column_value, serve_norm, fresh_query, fresh_key, fresh_value)
```

```python
import functools
import math

import jax
import jax.numpy as jnp
from jax import lax
from jax.experimental import pallas as pl
from jax.experimental.pallas import tpu as pltpu
from jax.sharding import PartitionSpec as P

keep_rate = 0.75
LANES = 128
CHUNK = 256
AHEAD = 3
LAG = 1
STEP = 64
MESH = pl.DeviceIdType.MESH


def row_step(rows):
    return math.gcd(rows, STEP)


def exchange(zero, tp, counts, width, *refs):
    (wq, aq, wk, ak, wv, av, train, step, fresh, serve, scales, gain,
     w_buf, a_buf, parts, read_sem, part_send, part_recv, send, recv, gain_send, gain_recv) = refs
    chunks = sum(counts)
    rows = wq.shape[0]
    me = lax.axis_index("zero")
    my_tp = lax.axis_index("tp")
    where = []
    for w, a, count in ((wq, aq, counts[0]), (wk, ak, counts[1]), (wv, av, counts[2])):
        where += [(w, a, j * width) for j in range(count)]

    def reads(c):
        w, a, at = where[c]
        return (
            pltpu.make_async_copy(w.at[:, pl.ds(at, width)], w_buf.at[c], read_sem.at[0, c]),
            pltpu.make_async_copy(a.at[:, pl.ds(at, width)], a_buf.at[c], read_sem.at[1, c]),
        )

    for c in range(min(AHEAD, chunks)):
        for copy in reads(c):
            copy.start()

    group = zero * tp
    mine = me * tp + my_tp

    def member(d):
        other = lax.rem(mine + d, group)
        return other, {"zero": other // tp, "tp": lax.rem(other, tp)}

    barrier = pltpu.get_barrier_semaphore()
    for d in range(1, group):
        pl.semaphore_signal(barrier, inc=1, device_id=member(d)[1], device_id_type=MESH)
    pl.semaphore_wait(barrier, group - 1)

    gain[mine] = train[...] + step[...]

    def part_copy(c, d):
        return pltpu.make_async_remote_copy(
            src_ref=parts.at[me, c], dst_ref=parts.at[me, c],
            send_sem=part_send.at[c, d - 1], recv_sem=part_recv.at[c, me],
            device_id={"zero": lax.rem(me + d, zero)}, device_id_type=MESH,
        )

    def part_arrival(c, d):
        other = lax.rem(me + d, zero)
        return pltpu.make_async_remote_copy(
            src_ref=parts.at[other, c], dst_ref=parts.at[other, c],
            send_sem=part_send.at[c, d - 1], recv_sem=part_recv.at[c, other],
            device_id={"zero": other}, device_id_type=MESH,
        )

    def block(c, owner):
        return serve.at[c, pl.ds(pl.multiple_of(owner * rows, rows), rows), :]

    def serve_copy(c, d):
        return pltpu.make_async_remote_copy(
            src_ref=block(c, me), dst_ref=block(c, me),
            send_sem=send.at[c, d - 1], recv_sem=recv.at[c, me],
            device_id={"zero": lax.rem(me + d, zero)}, device_id_type=MESH,
        )

    def serve_arrival(c, d):
        other = lax.rem(me + d, zero)
        return pltpu.make_async_remote_copy(
            src_ref=block(c, other), dst_ref=block(c, other),
            send_sem=send.at[c, d - 1], recv_sem=recv.at[c, other],
            device_id={"zero": other}, device_id_type=MESH,
        )

    def gain_copy(d):
        return pltpu.make_async_remote_copy(
            src_ref=gain.at[mine], dst_ref=gain.at[mine],
            send_sem=gain_send.at[d - 1], recv_sem=gain_recv.at[mine],
            device_id=member(d)[1], device_id_type=MESH,
        )

    def gain_arrival(d):
        other, place = member(d)
        return pltpu.make_async_remote_copy(
            src_ref=gain.at[other], dst_ref=gain.at[other],
            send_sem=gain_send.at[d - 1], recv_sem=gain_recv.at[other],
            device_id=place, device_id_type=MESH,
        )

    block_rows = row_step(rows)

    def mix(c):
        if c + AHEAD < chunks:
            for copy in reads(c + AHEAD):
                copy.start()
        for copy in reads(c):
            copy.wait()

        def one(i, total):
            at = pl.ds(pl.multiple_of(i * block_rows, block_rows), block_rows)
            new = keep_rate * a_buf[c, at, :] + (1.0 - keep_rate) * w_buf[c, at, :]
            fresh[c, at, :] = new
            return total + jnp.sum((new * new).reshape(block_rows // 8, 8, width), axis=0)

        total = lax.fori_loop(0, rows // block_rows, one, jnp.zeros((8, width), jnp.float32))
        parts[me, c] = jnp.sum(total, axis=0, keepdims=True)
        for d in range(1, zero):
            part_copy(c, d).start()

    def scale(c):
        for d in range(1, zero):
            part_arrival(c, d).wait_recv()
        total = parts[0, c]
        for k in range(1, zero):
            total = total + parts[k, c]
        column = jnp.sqrt(total)
        scales[c] = column
        inverse = jnp.broadcast_to(1.0 / column, (block_rows, width))

        def one(i, carry):
            at = pl.ds(pl.multiple_of(i * block_rows, block_rows), block_rows)
            to = pl.ds(pl.multiple_of(me * rows + i * block_rows, block_rows), block_rows)
            serve[c, to, :] = (fresh[c, at, :] * inverse).astype(jnp.bfloat16)
            return carry

        lax.fori_loop(0, rows // block_rows, one, 0)
        for d in range(1, zero):
            serve_copy(c, d).start()

    for c in range(chunks + LAG):
        if c < chunks:
            mix(c)
        if c == 0:
            for d in range(1, group):
                gain_copy(d).start()
        if c >= LAG:
            scale(c - LAG)

    for d in range(1, group):
        gain_copy(d).wait_send()
        gain_arrival(d).wait_recv()
    for c in range(chunks):
        for d in range(1, zero):
            part_copy(c, d).wait_send()
            serve_copy(c, d).wait_send()
            serve_arrival(c, d).wait_recv()


def place(counts, width, *refs):
    (fresh, serve, scales, gain, sq, sk, sv, cq, ck, cv, norm, fq, fk, fv, narrow, sem, norm_sem) = refs
    copies = []
    c = 0
    for full, column, own, count in ((sq, cq, fq, counts[0]), (sk, ck, fk, counts[1]), (sv, cv, fv, counts[2])):
        for j in range(count):
            at = pl.ds(j * width, width)
            copies.append(pltpu.make_async_copy(fresh.at[c], own.at[:, at], sem.at[0, c]))
            copies.append(pltpu.make_async_copy(serve.at[c], full.at[:, at], sem.at[1, c]))
            copies.append(pltpu.make_async_copy(scales.at[c], column.at[:, at], sem.at[2, c]))
            c += 1
    for copy in copies:
        copy.start()
    lanes = norm.shape[1]
    narrow[...] = gain[...].reshape(norm.shape[0], lanes).astype(jnp.bfloat16)
    copies.append(pltpu.make_async_copy(narrow, norm, norm_sem))
    copies[-1].start()
    for copy in copies:
        copy.wait()


def solution(mesh):
    zero, tp = mesh.shape["zero"], mesh.shape["tp"]
    group = zero * tp

    def body(w_query, avg_query, w_key, avg_key, w_value, avg_value, norm_train, norm_step):
        rows = w_query.shape[0]
        widths = [w.shape[1] for w in (w_query, w_key, w_value)]
        width = math.gcd(CHUNK, *widths)
        counts = tuple(w // width for w in widths)
        chunks = sum(counts)
        piece = norm_train.shape[0]
        lanes = math.gcd(piece, LANES)
        f32, bf16 = jnp.float32, jnp.bfloat16
        hbm = pl.BlockSpec(memory_space=pl.ANY)
        vmem = pl.BlockSpec(memory_space=pltpu.VMEM)
        dma = pltpu.SemaphoreType.DMA
        staged = 2 * chunks * rows * width * 4
        others = max(zero - 1, 1)
        results = pl.pallas_call(
            functools.partial(exchange, zero, tp, counts, width),
            out_shape=(
                pltpu.VMEM((chunks, rows, width), f32),
                pltpu.VMEM((chunks, zero * rows, width), bf16),
                pltpu.VMEM((chunks, 1, width), f32),
                pltpu.VMEM((group, piece // lanes, lanes), f32),
            ),
            in_specs=[hbm] * 6 + [vmem] * 2,
            out_specs=(vmem,) * 4,
            scratch_shapes=[
                pltpu.VMEM((chunks, rows, width), f32),
                pltpu.VMEM((chunks, rows, width), f32),
                pltpu.VMEM((zero, chunks, 1, width), f32),
                dma((2, chunks)),
                dma((chunks, others)),
                dma((chunks, zero)),
                dma((chunks, others)),
                dma((chunks, zero)),
                dma((max(group - 1, 1),)),
                dma((group,)),
            ],
            compiler_params=pltpu.CompilerParams(
                collective_id=0, has_side_effects=True, vmem_limit_bytes=staged + (4 << 20)
            ),
        )(
            w_query, avg_query, w_key, avg_key, w_value, avg_value,
            norm_train.reshape(-1, lanes), norm_step.reshape(-1, lanes),
        )
        shape = jax.ShapeDtypeStruct
        outs = pl.pallas_call(
            functools.partial(place, counts, width),
            out_shape=(
                *(shape((zero * rows, w), bf16) for w in widths),
                *(shape((1, w), f32) for w in widths),
                shape((group * piece // lanes, lanes), bf16),
                *(shape((rows, w), f32) for w in widths),
            ),
            in_specs=[vmem] * 4,
            out_specs=(hbm,) * 10,
            scratch_shapes=[
                pltpu.VMEM((group * piece // lanes, lanes), bf16),
                dma((3, chunks)),
                dma,
            ],
            compiler_params=pltpu.CompilerParams(vmem_limit_bytes=2 << 20),
        )(*results)
        sq, sk, sv, cq, ck, cv, norm, fq, fk, fv = outs
        return sq, sk, sv, cq.reshape(-1), ck.reshape(-1), cv.reshape(-1), norm.reshape(-1), fq, fk, fv

    weights = P(("job", "zero"), "tp")
    in_specs = (weights,) * 6 + (P(("job", "zero", "tp")),) * 2
    out_specs = (P("job", "tp"),) * 3 + (P(("job", "tp")),) * 3 + (P("job"),) + (weights,) * 3
    return jax.shard_map(body, mesh=mesh, in_specs=in_specs, out_specs=out_specs, check_vma=False)
```

```python
import functools
import math

import jax
import jax.numpy as jnp
from jax import lax
from jax.experimental import pallas as pl
from jax.experimental.pallas import tpu as pltpu
from jax.sharding import PartitionSpec as P

keep_rate = 0.75
LANES = 128
CHUNK = 256
AHEAD = 3
SPLIT = 2
LAG = 1
STEP = 128
MESH = pl.DeviceIdType.MESH


def row_step(rows):
    return math.gcd(rows, STEP)


def exchange(zero, tp, counts, width, *refs):
    (wq, aq, wk, ak, wv, av, train, step, fresh, serve, scales, gain,
     w_buf, a_buf, norm_buf, parts, read_sem, norm_sem, part_send, part_recv, send, recv, gain_send, gain_recv) = refs
    rows = wq.shape[0]
    me = lax.axis_index("zero")
    my_tp = lax.axis_index("tp")
    where = []
    for w, a, count in ((wq, aq, counts[0]), (wk, ak, counts[1]), (wv, av, counts[2])):
        where += [(w, a, j * width) for j in range(count)]
    cuts = []
    for c in range(len(where)):
        parted = SPLIT if c == 0 and width % (SPLIT * LANES) == 0 else 1
        cuts += [(c, k * (width // parted), width // parted) for k in range(parted)]
    pieces = len(cuts)

    def cut(c):
        chunk, sub, wide = cuts[c]
        return chunk, pl.ds(sub, wide), wide

    def reads(c):
        chunk, sub, wide = cuts[c]
        w, a, at = where[chunk]
        here, there = pl.ds(at + sub, wide), pl.ds(sub, wide)
        return (
            pltpu.make_async_copy(w.at[:, here], w_buf.at[chunk, :, there], read_sem.at[0, c]),
            pltpu.make_async_copy(a.at[:, here], a_buf.at[chunk, :, there], read_sem.at[1, c]),
        )

    for c in range(min(AHEAD, pieces)):
        for copy in reads(c):
            copy.start()
    norm_reads = [
        pltpu.make_async_copy(ref, norm_buf.at[k], norm_sem.at[k]) for k, ref in enumerate((train, step))
    ]
    for copy in norm_reads:
        copy.start()

    group = zero * tp
    mine = me * tp + my_tp

    def member(d):
        other = lax.rem(mine + d, group)
        return other, {"zero": other // tp, "tp": lax.rem(other, tp)}

    barrier = pltpu.get_barrier_semaphore()
    for d in range(1, group):
        pl.semaphore_signal(barrier, inc=1, device_id=member(d)[1], device_id_type=MESH)
    pl.semaphore_wait(barrier, group - 1)


    def sums(c, owner):
        chunk, at, _ = cut(c)
        return parts.at[owner, chunk, :, at]

    def part_copy(c, d):
        return pltpu.make_async_remote_copy(
            src_ref=sums(c, me), dst_ref=sums(c, me),
            send_sem=part_send.at[c, d - 1], recv_sem=part_recv.at[c, me],
            device_id={"zero": lax.rem(me + d, zero)}, device_id_type=MESH,
        )

    def part_arrival(c, d):
        other = lax.rem(me + d, zero)
        return pltpu.make_async_remote_copy(
            src_ref=sums(c, other), dst_ref=sums(c, other),
            send_sem=part_send.at[c, d - 1], recv_sem=part_recv.at[c, other],
            device_id={"zero": other}, device_id_type=MESH,
        )

    def block(c, owner):
        chunk, at, _ = cut(c)
        return serve.at[chunk, pl.ds(pl.multiple_of(owner * rows, rows), rows), at]

    def serve_copy(c, d):
        return pltpu.make_async_remote_copy(
            src_ref=block(c, me), dst_ref=block(c, me),
            send_sem=send.at[c, d - 1], recv_sem=recv.at[c, me],
            device_id={"zero": lax.rem(me + d, zero)}, device_id_type=MESH,
        )

    def serve_arrival(c, d):
        other = lax.rem(me + d, zero)
        return pltpu.make_async_remote_copy(
            src_ref=block(c, other), dst_ref=block(c, other),
            send_sem=send.at[c, d - 1], recv_sem=recv.at[c, other],
            device_id={"zero": other}, device_id_type=MESH,
        )

    def gain_copy(d):
        return pltpu.make_async_remote_copy(
            src_ref=gain.at[mine], dst_ref=gain.at[mine],
            send_sem=gain_send.at[d - 1], recv_sem=gain_recv.at[mine],
            device_id=member(d)[1], device_id_type=MESH,
        )

    def gain_arrival(d):
        other, place = member(d)
        return pltpu.make_async_remote_copy(
            src_ref=gain.at[other], dst_ref=gain.at[other],
            send_sem=gain_send.at[d - 1], recv_sem=gain_recv.at[other],
            device_id=place, device_id_type=MESH,
        )

    block_rows = row_step(rows)

    def mix(c):
        if c + AHEAD < pieces:
            for copy in reads(c + AHEAD):
                copy.start()
        for copy in reads(c):
            copy.wait()
        chunk, columns, wide = cut(c)

        def one(i, total):
            at = pl.ds(pl.multiple_of(i * block_rows, block_rows), block_rows)
            new = keep_rate * a_buf[chunk, at, columns] + (1.0 - keep_rate) * w_buf[chunk, at, columns]
            fresh[chunk, at, columns] = new
            return total + jnp.sum((new * new).reshape(block_rows // 8, 8, wide), axis=0)

        total = lax.fori_loop(0, rows // block_rows, one, jnp.zeros((8, wide), jnp.float32))
        parts[me, chunk, :, columns] = jnp.sum(total, axis=0, keepdims=True)
        for d in range(1, zero):
            part_copy(c, d).start()

    def scale(c):
        for d in range(1, zero):
            part_arrival(c, d).wait_recv()
        chunk, columns, wide = cut(c)
        total = parts[0, chunk, :, columns]
        for k in range(1, zero):
            total = total + parts[k, chunk, :, columns]
        column = jnp.sqrt(total)
        scales[chunk, :, columns] = column
        inverse = jnp.broadcast_to(1.0 / column, (block_rows, wide))

        def one(i, carry):
            at = pl.ds(pl.multiple_of(i * block_rows, block_rows), block_rows)
            to = pl.ds(pl.multiple_of(me * rows + i * block_rows, block_rows), block_rows)
            serve[chunk, to, columns] = (fresh[chunk, at, columns] * inverse).astype(jnp.bfloat16)
            return carry

        lax.fori_loop(0, rows // block_rows, one, 0)
        for d in range(1, zero):
            serve_copy(c, d).start()

    for c in range(pieces + LAG):
        if c < pieces:
            mix(c)
        if c == 0:
            for copy in norm_reads:
                copy.wait()
            gain[mine] = norm_buf[0] + norm_buf[1]
            for d in range(1, group):
                gain_copy(d).start()
        if c >= LAG:
            scale(c - LAG)

    for d in range(1, group):
        gain_copy(d).wait_send()
        gain_arrival(d).wait_recv()
    for c in range(pieces):
        for d in range(1, zero):
            part_copy(c, d).wait_send()
            serve_copy(c, d).wait_send()
            serve_arrival(c, d).wait_recv()


def place(counts, width, *refs):
    (fresh, serve, scales, gain, sq, sk, sv, cq, ck, cv, norm, fq, fk, fv, narrow, sem, norm_sem) = refs
    copies = []
    c = 0
    for full, column, own, count in ((sq, cq, fq, counts[0]), (sk, ck, fk, counts[1]), (sv, cv, fv, counts[2])):
        for j in range(count):
            at = pl.ds(j * width, width)
            copies.append(pltpu.make_async_copy(fresh.at[c], own.at[:, at], sem.at[0, c]))
            copies.append(pltpu.make_async_copy(serve.at[c], full.at[:, at], sem.at[1, c]))
            copies.append(pltpu.make_async_copy(scales.at[c], column.at[:, at], sem.at[2, c]))
            c += 1
    for copy in copies:
        copy.start()
    lanes = norm.shape[1]
    narrow[...] = gain[...].reshape(norm.shape[0], lanes).astype(jnp.bfloat16)
    copies.append(pltpu.make_async_copy(narrow, norm, norm_sem))
    copies[-1].start()
    for copy in copies:
        copy.wait()


def solution(mesh):
    zero, tp = mesh.shape["zero"], mesh.shape["tp"]
    group = zero * tp

    def body(w_query, avg_query, w_key, avg_key, w_value, avg_value, norm_train, norm_step):
        rows = w_query.shape[0]
        widths = [w.shape[1] for w in (w_query, w_key, w_value)]
        width = math.gcd(CHUNK, *widths)
        counts = tuple(w // width for w in widths)
        chunks = sum(counts)
        piece = norm_train.shape[0]
        lanes = math.gcd(piece, LANES)
        f32, bf16 = jnp.float32, jnp.bfloat16
        hbm = pl.BlockSpec(memory_space=pltpu.HBM)
        hold = lambda x: pltpu.with_memory_space_constraint(x, pltpu.HBM)
        vmem = pl.BlockSpec(memory_space=pltpu.VMEM)
        dma = pltpu.SemaphoreType.DMA
        staged = 2 * chunks * rows * width * 4
        others = max(zero - 1, 1)
        results = pl.pallas_call(
            functools.partial(exchange, zero, tp, counts, width),
            out_shape=(
                pltpu.VMEM((chunks, rows, width), f32),
                pltpu.VMEM((chunks, zero * rows, width), bf16),
                pltpu.VMEM((chunks, 1, width), f32),
                pltpu.VMEM((group, piece // lanes, lanes), f32),
            ),
            in_specs=[hbm] * 8,
            out_specs=(vmem,) * 4,
            scratch_shapes=[
                pltpu.VMEM((chunks, rows, width), f32),
                pltpu.VMEM((chunks, rows, width), f32),
                pltpu.VMEM((2, piece // lanes, lanes), f32),
                pltpu.VMEM((zero, chunks, 1, width), f32),
                dma((2, chunks + SPLIT)),
                dma((2,)),
                dma((chunks + SPLIT, others)),
                dma((chunks + SPLIT, zero)),
                dma((chunks + SPLIT, others)),
                dma((chunks + SPLIT, zero)),
                dma((max(group - 1, 1),)),
                dma((group,)),
            ],
            compiler_params=pltpu.CompilerParams(
                collective_id=0, has_side_effects=True, vmem_limit_bytes=staged + (4 << 20)
            ),
        )(
            *map(hold, (w_query, avg_query, w_key, avg_key, w_value, avg_value)),
            hold(norm_train.reshape(-1, lanes)), hold(norm_step.reshape(-1, lanes)),
        )
        shape = jax.ShapeDtypeStruct
        outs = pl.pallas_call(
            functools.partial(place, counts, width),
            out_shape=(
                *(shape((zero * rows, w), bf16) for w in widths),
                *(shape((1, w), f32) for w in widths),
                shape((group * piece // lanes, lanes), bf16),
                *(shape((rows, w), f32) for w in widths),
            ),
            in_specs=[vmem] * 4,
            out_specs=(hbm,) * 10,
            scratch_shapes=[
                pltpu.VMEM((group * piece // lanes, lanes), bf16),
                dma((3, chunks)),
                dma,
            ],
            compiler_params=pltpu.CompilerParams(vmem_limit_bytes=2 << 20),
        )(*results)
        sq, sk, sv, cq, ck, cv, norm, fq, fk, fv = outs
        return sq, sk, sv, cq.reshape(-1), ck.reshape(-1), cv.reshape(-1), norm.reshape(-1), fq, fk, fv

    weights = P(("job", "zero"), "tp")
    in_specs = (weights,) * 6 + (P(("job", "zero", "tp")),) * 2
    out_specs = (P("job", "tp"),) * 3 + (P(("job", "tp")),) * 3 + (P("job"),) + (weights,) * 3
    return jax.shard_map(body, mesh=mesh, in_specs=in_specs, out_specs=out_specs, check_vma=False)
```
